32 devices in a mesh: gx: 8 (over z, x), gy: 4 (over y, core).
Axes of the slice: x: 2, y: 2, z: 4, core: 2. Of those that a mesh axis runs over, the one named last changes fastest.
Arguments:
- vectors: float32 [8, 2, 2, 128, 1024], P(None, None, None, 'gx', 'gy'), may hold values from -6 to 6
- bonds: float32 [3, 128, 1024], P(None, 'gx', 'gy'), may hold values from 0.5 to 1.5
- onsite: float32 [2, 128, 1024], P(None, 'gx', 'gy'), may hold values from -1 to 1
Outputs:
- moment_rows: float32 [2, 3, 3, 128], P(None, None, None, 'gx')
- left_last: bfloat16 [8, 2, 2, 128, 1024], P(None, None, None, 'gx', 'gy')
- right_last: bfloat16 [8, 2, 2, 128, 1024], P(None, None, None, 'gx', 'gy')
The draws below stay inside these ranges and needn't reach their ends.
All inputs are finite; a program needn't handle non-finite values.
Results may differ from the reference program's by a relative error of at most 0.001.
Values sent between devices are 32-bit elements; how exact they have to be, the bound alone decides.
A program may use at most 64 MiB of HBM per device.

```python
import math
import jax
import jax.numpy as jnp

VECTORS = 8
MOMENTS = 3
NX = 128
NY = 1024


def block_scale(stream_key, shape, shards, low, top_value):
    def one(position, blocks):
        draws = jax.random.uniform(jax.random.fold_in(jax.random.fold_in(stream_key, 6), position), (blocks,), jnp.float32, low / len(shards), top_value / len(shards))
        return jnp.repeat(jnp.exp(draws), shape[position] // blocks).reshape((-1,) + (1,) * (len(shape) - position - 1))

    gain = one(*shards[0])
    for cut in shards[1:]:
        gain = gain * one(*cut)
    return gain


def scatter_about(stream_key, dims, scale, limit, split=(), dtype=jnp.bfloat16):
    gain = block_scale(stream_key, dims, split, -0.22, 0.18) if split else 1.0
    array = jax.random.normal(stream_key, dims, jnp.float32) * scale * gain
    return jnp.minimum(jnp.maximum(array, -limit), limit).astype(dtype)


def setup_inputs(seed: int = 0) -> dict:
    seeds = jax.random.split(jax.random.key(seed), 4)
    vectors = scatter_about(seeds[0], (VECTORS, 2, 2, NX, NY), 1.0, 6.0, ((3, 8), (4, 4)), jnp.float32)
    bonds = jnp.clip(jnp.exp(math.log(1.5) - 1.0986123 * jax.random.uniform(seeds[1], (3, NX, NY), jnp.float32) ** block_scale(seeds[1], (3, NX, NY), ((1, 8), (2, 4)), -0.2, 0.2)), 0.5, 1.5)
    onsite = jnp.clip(jax.random.uniform(seeds[2], (2, NX, NY), jnp.float32, -1.0, 1.0) * block_scale(seeds[2], (2, NX, NY), ((1, 8), (2, 4)), -0.4, 0.0), -1.0, 1.0)
    return {"vectors": vectors, "bonds": bonds, "onsite": onsite}


SCALE = 6.0
OFFSETS = (1.0, -0.5, -0.5)
UNITS = (1.0, 1.0, 1.0)


def bond_sums(vector_field, bonds, weights):
    site_a = vector_field[:, :, 0]
    site_b = vector_field[:, :, 1]
    raised_one = jnp.roll(bonds[1], -1, 0)
    raised_two = jnp.roll(bonds[2], -1, 1)
    into_a = (weights[0] * bonds[0] * site_b
              + weights[1] * bonds[1] * jnp.roll(site_b, 1, 2)
              + weights[2] * bonds[2] * jnp.roll(site_b, 1, 3))
    into_b = (weights[0] * bonds[0] * site_a
              + weights[1] * raised_one * jnp.roll(site_a, -1, 2)
              + weights[2] * raised_two * jnp.roll(site_a, -1, 3))
    return site_a, site_b, into_a, into_b


def hamilton(vector_field, bonds, onsite):
    site_a, site_b, into_a, into_b = bond_sums(vector_field, bonds, UNITS)
    return jnp.stack([(onsite[0] * site_a + into_a) / SCALE,
                      (onsite[1] * site_b + into_b) / SCALE], axis=2)


def velocity(vector_field, bonds):
    site_a, site_b, sum_a, sum_b = bond_sums(vector_field, bonds, OFFSETS)
    image_a = jnp.stack([sum_a[:, 1], -sum_a[:, 0]], axis=1)
    image_b = jnp.stack([-sum_b[:, 1], sum_b[:, 0]], axis=1)
    return jnp.stack([image_a, image_b], axis=2)


def intersection(left, right):
    real_rows = jnp.sum(left[:, 0] * right[:, 0] + left[:, 1] * right[:, 1], axis=(0, 1, 3))
    imag_rows = jnp.sum(left[:, 0] * right[:, 1] - left[:, 1] * right[:, 0], axis=(0, 1, 3))
    return jnp.stack([real_rows, imag_rows])


def reference(vectors, bonds, onsite):
    right_chain = [vectors]
    for level in range(1, MOMENTS):
        stepped = hamilton(right_chain[level - 1], bonds, onsite)
        right_chain.append(stepped if level == 1 else 2.0 * stepped - right_chain[level - 2])
    rights = [velocity(entry, bonds) for entry in right_chain]
    lefts = [rights[0]]
    for level in range(1, MOMENTS):
        stepped = hamilton(lefts[level - 1], bonds, onsite)
        lefts.append(stepped if level == 1 else 2.0 * stepped - lefts[level - 2])
    moments = jnp.stack([jnp.stack([intersection(lefts[order], rights[other]) for other in range(MOMENTS)], axis=1)
                         for order in range(MOMENTS)], axis=1)
    moments = moments / float(VECTORS * NY)
    return moments, lefts[-1].astype(jnp.bfloat16), rights[-1].astype(jnp.bfloat16)
```

```python
import functools
import jax
import jax.numpy as jnp
from jax import lax
from jax.experimental import pallas as pl
from jax.experimental.pallas import tpu as pltpu
from jax.sharding import PartitionSpec as P

MOMENTS = 3
SCALE = 6.0
EDGE = 2
GROUP = 4
HALF = 64
LANES = 128
MESH = pl.DeviceIdType.MESH


def bond_terms(a, b, fields, left, right, up, down):
    b0, b1, b2, b1d, b2r = fields
    return b0 * b, b1 * up(b) + b2 * left(b), b0 * a, b1d * down(a) + b2r * right(a)


def kernel(
    gxn, gyn, vec, bonds, onsite, out_mom, out_left, out_right,
    x, f, fd, c_own, c_left, c_right, halo_f, halo_x, keep, acc, part_mom, lbuf, rbuf,
    load_sem, send_sem, recv_sem, msend_sem, mrecv_sem, out_sem,
):
    vectors, _, _, rows, cols = vec.shape
    tall = x.shape[3]
    tiles = cols // LANES
    last = rows - EDGE
    gx = lax.axis_index("gx")
    gy = lax.axis_index("gy")

    def peer(dx, dy):
        return (lax.rem(gx + dx + gxn, gxn), lax.rem(gy + dy + gyn, gyn))

    barrier = pltpu.get_barrier_semaphore()
    near = [(dx % gxn, dy % gyn) for dx in (-1, 0, 1) for dy in (-1, 0, 1)]
    near += [(0, dy) for dy in range(gyn)]
    near = sorted(set(near) - {(0, 0)})
    for dx, dy in near:
        pl.semaphore_signal(barrier, inc=1, device_id=peer(dx, dy), device_id_type=MESH)

    loads = [
        pltpu.make_async_copy(vec, x.at[:, :, :, 0:rows, :], load_sem.at[0]),
        pltpu.make_async_copy(bonds, f.at[0:3, 0:rows, :], load_sem.at[1]),
        pltpu.make_async_copy(onsite, f.at[3:5, 0:rows, :], load_sem.at[2]),
    ]
    for copy in loads:
        copy.start()
    pl.semaphore_wait(barrier, len(near))

    sends = []

    def send(src, dst, dx, dy):
        n = len(sends)
        copy = pltpu.make_async_remote_copy(
            src_ref=src, dst_ref=dst, send_sem=send_sem.at[n], recv_sem=recv_sem.at[n],
            device_id=peer(dx, dy), device_id_type=MESH,
        )
        copy.start()
        sends.append(copy)

    below = slice(rows, rows + EDGE)
    send(vec.at[:, :, 0, 0:2, :], x.at[:, :, 0, rows : rows + 2, :], -1, 0)
    send(vec.at[:, :, 1, rows - 2 : rows, :], x.at[:, :, 1, tall - 2 : tall, :], 1, 0)
    send(vec.at[:, :, 1, 0:1, :], x.at[:, :, 1, rows : rows + 1, :], -1, 0)
    send(vec.at[:, :, 0, rows - 1 : rows, :], x.at[:, :, 0, tall - 1 : tall, :], 1, 0)
    send(bonds.at[:, 0:2, :], f.at[0:3, rows : rows + 2, :], -1, 0)
    send(bonds.at[:, rows - 2 : rows, :], f.at[0:3, tall - 2 : tall, :], 1, 0)
    send(onsite.at[:, 0:2, :], f.at[3:5, rows : rows + 2, :], -1, 0)
    send(onsite.at[:, rows - 2 : rows, :], f.at[3:5, tall - 2 : tall, :], 1, 0)

    for copy in loads:
        copy.wait()

    lane = lax.broadcasted_iota(jnp.int32, (rows, LANES), 1)
    spot = lax.rem(lane, HALF)

    def packed(items):
        total = jnp.zeros((rows, LANES), jnp.float32)
        for k, (first, final) in enumerate(items):
            both = jnp.where(lane < HALF, first, final)
            moved = pltpu.roll(both, GROUP * k + EDGE, 1)
            total = jnp.where(spot // GROUP == k, moved, total) if k else moved
        total = jnp.where(lane < HALF, total, pltpu.roll(total, HALF, 1))
        return total

    def edges(ref, *index):
        return ref[(*index, slice(0, rows), slice(0, LANES))], ref[
            (*index, slice(0, rows), slice(cols - LANES, cols))
        ]

    for sub in range(2):
        c_own[sub, 0:rows] = packed(
            [edges(x, v, p, sub) for v in range(vectors) for p in range(2)]
        )
    c_own[2, 0:rows] = packed([edges(f, k) for k in range(5)])

    core = slice(0, rows)
    send(c_own.at[:, core, :], c_right.at[:, core, :], 0, -1)
    send(c_own.at[:, core, :], c_left.at[:, core, :], 0, 1)
    top, bottom = c_own.at[:, 0:EDGE, :], c_own.at[:, last:rows, :]
    past, ahead = slice(rows, rows + EDGE), slice(tall - EDGE, tall)
    send(top, c_own.at[:, past, :], -1, 0)
    send(top, c_right.at[:, past, :], -1, -1)
    send(top, c_left.at[:, past, :], -1, 1)
    send(bottom, c_own.at[:, ahead, :], 1, 0)
    send(bottom, c_right.at[:, ahead, :], 1, -1)
    send(bottom, c_left.at[:, ahead, :], 1, 1)

    acc[...] = jnp.zeros_like(acc)
    for copy in sends:
        copy.wait_recv()

    tlane = lax.broadcasted_iota(jnp.int32, (tall, LANES), 1)
    tspot = lax.rem(tlane, GROUP)
    from_left = (tlane < HALF) & (tspot < EDGE)
    from_right = (tlane >= HALF) & (tspot >= EDGE)

    def joined(k):
        return jnp.where(
            from_left, c_left[k], jnp.where(from_right, c_right[k], c_own[k])
        )

    def up(t):
        return pltpu.roll(t, 1, 0)

    def down(t):
        return pltpu.roll(t, t.shape[0] - 1, 0)

    field_tile = joined(2)
    tgroup = lax.rem(tlane, HALF)
    for k in range(5):
        t = pltpu.roll(field_tile, LANES - GROUP * k, 1) if k else field_tile
        t = jnp.where(tgroup < GROUP, t, 0.0)
        step = GROUP
        while step < HALF:
            t = t + pltpu.roll(t, step, 1)
            step *= 2
        halo_f[k] = t
    halo_f[5] = down(halo_f[1])
    halo_f[6] = pltpu.roll(halo_f[2], LANES - 1, 1)

    lane_last = tlane == LANES - 1
    lane_first = tlane == 0

    def tile(t):
        return slice(t * LANES, (t + 1) * LANES)

    for t in range(tiles):
        fd[0, :, tile(t)] = down(f[1, :, tile(t)])
    after = pltpu.roll(halo_f[2], LANES - 1 - (HALF + EDGE), 1)
    for t in reversed(range(tiles)):
        turned = pltpu.roll(f[2, :, tile(t)], LANES - 1, 1)
        fd[1, :, tile(t)] = jnp.where(lane_last, after, turned)
        after = turned

    sixth = 1.0 / SCALE

    def h_fields(width=tall):
        return tuple(halo_f[k] for k in (0, 1, 2, 5, 6))

    h_on = (halo_f[3], halo_f[4])

    def h_terms(a, b):
        return bond_terms(
            a, b, h_fields(), lambda t: pltpu.roll(t, 1, 1),
            lambda t: pltpu.roll(t, LANES - 1, 1), up, down,
        )

    def energy(a, b, terms, on, factor):
        a0, a12, b0, b12 = terms
        return (on[0] * a + (a0 + a12)) * factor, (on[1] * b + (b0 + b12)) * factor

    def speed(terms):
        a0, a12, b0, b12 = terms
        return a0 - 0.5 * a12, 0.5 * b12 - b0

    q0 = (joined(0), joined(1))
    t0 = h_terms(*q0)
    q1 = energy(*q0, t0, h_on, sixth)
    m0 = speed(t0)
    h1 = energy(*q1, h_terms(*q1), h_on, 2.0 * sixth)
    q2 = (h1[0] - q0[0], h1[1] - q0[1])
    m1 = energy(*m0, h_terms(*m0), h_on, sixth)
    for k, pair in enumerate((q0, q1, q2, m0, m1)):
        halo_x[k, 0], halo_x[k, 1] = pair

    short = slice(0, rows)

    def one_vector(v, carry):
        for part in range(2):
            turn_b = lax.rem(2 * LANES - (GROUP * (2 * v + part) + 1), LANES)
            turn_a = lax.rem(3 * LANES - 1 - (HALF + GROUP * (2 * v + part) + EDGE), LANES)

            def terms(pair, k, cut):
                a, b = pair
                rim_b = pltpu.roll(halo_x[k, 1], turn_b, 1)
                rim_a = pltpu.roll(halo_x[k, 0], turn_a, 1)
                keep_rows = (lambda t: t[0:rows]) if cut else (lambda t: t)
                first, final = keep_rows(lane_first), keep_rows(lane_last)
                size = short if cut else slice(0, tall)
                b_turn = [pltpu.roll(keep_rows(t), 1, 1) for t in b]
                a_turn = [pltpu.roll(keep_rows(t), LANES - 1, 1) for t in a]
                found = []
                for t in range(tiles):
                    prev = keep_rows(rim_b) if t == 0 else b_turn[t - 1]
                    nxt = keep_rows(rim_a) if t == tiles - 1 else a_turn[t + 1]
                    left = jnp.where(first, prev, b_turn[t])
                    right = jnp.where(final, nxt, a_turn[t])
                    a0 = f[0, size, tile(t)] * keep_rows(b[t])
                    a12 = f[1, size, tile(t)] * keep_rows(up(b[t])) + f[2, size, tile(t)] * left
                    b0 = f[0, size, tile(t)] * keep_rows(a[t])
                    b12 = fd[0, size, tile(t)] * keep_rows(down(a[t])) + fd[1, size, tile(t)] * right
                    found.append((a0, a12, b0, b12))
                return found

            def stepped(pair, found, factor, cut, minus=None):
                a_new, b_new = [], []
                size = short if cut else slice(0, tall)
                for t in range(tiles):
                    on = (f[3, size, tile(t)], f[4, size, tile(t)])
                    a, b = energy(pair[0][t][size], pair[1][t][size], found[t], on, factor)
                    if minus is not None:
                        a, b = a - minus[0][t][size], b - minus[1][t][size]
                    a_new.append(a)
                    b_new.append(b)
                return a_new, b_new

            def moved(found):
                both = [speed(item) for item in found]
                return [item[0] for item in both], [item[1] for item in both]

            def store(slot, pair):
                for sub in range(2):
                    for t in range(tiles):
                        keep[slot, part, sub, :, tile(t)] = pair[sub][t][0:rows]

            q0 = tuple([x[v, part, sub, :, tile(t)] for t in range(tiles)] for sub in range(2))
            t0 = terms(q0, 0, False)
            m0 = moved(t0)
            store(0, m0)
            q1 = stepped(q0, t0, sixth, False)
            t1 = terms(q1, 1, False)
            store(3, moved(t1))
            q2 = stepped(q1, t1, 2.0 * sixth, False, q0)
            n2 = moved(terms(q2, 2, True))
            store(4, n2)
            m1 = stepped(m0, terms(m0, 3, False), sixth, False)
            store(1, m1)
            m2 = stepped(m1, terms(m1, 4, True), 2.0 * sixth, True, m0)
            store(2, m2)
            for sub in range(2):
                for t in range(tiles):
                    for buf, pair in ((lbuf, m2), (rbuf, n2)):
                        value = pair[sub][t]
                        value = -value if part == 0 else value
                        buf[v, 1 - part, sub, :, tile(t)] = value.astype(jnp.bfloat16)

        for r in range(0, rows, 8):
            band = slice(r, r + 8)
            sums = [[[acc[p, n, m, band, :] for m in range(MOMENTS)] for n in range(MOMENTS)] for p in range(2)]
            for sub in range(2):
                for t in range(tiles):
                    at = [[keep[s, p, sub, band, tile(t)] for p in range(2)] for s in range(5)]
                    for n in range(MOMENTS):
                        for m in range(MOMENTS):
                            left = at[n]
                            right = at[0] if m == 0 else at[2 + m]
                            sums[0][n][m] = sums[0][n][m] + (left[0] * right[0] + left[1] * right[1])
                            sums[1][n][m] = sums[1][n][m] + (left[0] * right[1] - left[1] * right[0])
            for p in range(2):
                for n in range(MOMENTS):
                    for m in range(MOMENTS):
                        acc[p, n, m, band, :] = sums[p][n][m]
        return carry

    lax.fori_loop(0, vectors, one_vector, 0)

    outs = [
        pltpu.make_async_copy(lbuf, out_left, out_sem.at[0]),
        pltpu.make_async_copy(rbuf, out_right, out_sem.at[1]),
    ]
    for copy in outs:
        copy.start()

    count = 2 * MOMENTS * MOMENTS * rows
    part_mom[0] = lax.dot_general(
        jnp.ones((8, LANES), jnp.float32), acc[...].reshape(count, LANES),
        (((1,), (1,)), ((), ())), precision=lax.Precision.HIGHEST,
        preferred_element_type=jnp.float32,
    )
    swaps = []
    for d in range(1, gyn):
        copy = pltpu.make_async_remote_copy(
            src_ref=part_mom.at[0], dst_ref=part_mom.at[d],
            send_sem=msend_sem.at[d - 1], recv_sem=mrecv_sem.at[d - 1],
            device_id=peer(0, d), device_id_type=MESH,
        )
        copy.start()
        swaps.append(copy)
    for copy in swaps:
        copy.wait_recv()
    total = part_mom[0]
    for d in range(1, gyn):
        total = total + part_mom[d]
    total = total / float(vectors * cols * gyn)
    for p in range(2):
        for n in range(MOMENTS):
            for m in range(MOMENTS):
                k = (p * MOMENTS + n) * MOMENTS + m
                out_mom[p, n, m : m + 1, :] = total[0:1, k * rows : (k + 1) * rows]
    for copy in sends + swaps:
        copy.wait_send()
    for copy in outs:
        copy.wait()


def solution(mesh):
    gxn, gyn = mesh.shape["gx"], mesh.shape["gy"]

    def per_device(vectors, bonds, onsite):
        count, _, _, rows, cols = vectors.shape
        tall = rows + 8
        f32 = jnp.float32
        any_space = pl.BlockSpec(memory_space=pl.ANY)
        last = jax.ShapeDtypeStruct(vectors.shape, jnp.bfloat16)
        sends = 16
        return pl.pallas_call(
            functools.partial(kernel, gxn, gyn),
            out_shape=(
                jax.ShapeDtypeStruct((2, MOMENTS, MOMENTS, rows), f32), last, last,
            ),
            in_specs=[any_space] * 3,
            out_specs=(pl.BlockSpec(memory_space=pltpu.VMEM), any_space, any_space),
            scratch_shapes=[
                pltpu.VMEM((count, 2, 2, tall, cols), f32),
                pltpu.VMEM((5, tall, cols), f32),
                pltpu.VMEM((2, tall, cols), f32),
                pltpu.VMEM((3, tall, LANES), f32),
                pltpu.VMEM((3, tall, LANES), f32),
                pltpu.VMEM((3, tall, LANES), f32),
                pltpu.VMEM((7, tall, LANES), f32),
                pltpu.VMEM((5, 2, tall, LANES), f32),
                pltpu.VMEM((5, 2, 2, rows, cols), f32),
                pltpu.VMEM((2, MOMENTS, MOMENTS, rows, LANES), f32),
                pltpu.VMEM((gyn, 8, 2 * MOMENTS * MOMENTS * rows), f32),
                pltpu.VMEM(vectors.shape, jnp.bfloat16),
                pltpu.VMEM(vectors.shape, jnp.bfloat16),
                pltpu.SemaphoreType.DMA((3,)),
                pltpu.SemaphoreType.DMA((sends,)),
                pltpu.SemaphoreType.DMA((sends,)),
                pltpu.SemaphoreType.DMA((gyn - 1,)),
                pltpu.SemaphoreType.DMA((gyn - 1,)),
                pltpu.SemaphoreType.DMA((2,)),
            ],
            compiler_params=pltpu.CompilerParams(collective_id=0, has_side_effects=True),
        )(vectors, bonds, onsite)

    return jax.shard_map(
        per_device,
        mesh=mesh,
        in_specs=(P(None, None, None, "gx", "gy"), P(None, "gx", "gy"), P(None, "gx", "gy")),
        out_specs=(
            P(None, None, None, "gx"),
            P(None, None, None, "gx", "gy"),
            P(None, None, None, "gx", "gy"),
        ),
        check_vma=False,
    )
```

```python
import functools
import jax
import jax.numpy as jnp
from jax import lax
from jax.experimental import pallas as pl
from jax.experimental.pallas import tpu as pltpu
from jax.sharding import PartitionSpec as P

MOMENTS = 3
SCALE = 6.0
EDGE = 2
GROUP = 4
HALF = 64
LANES = 128
GRANT = 16 * 1024 * 1024
MESH = pl.DeviceIdType.MESH


def bond_terms(a, b, fields, left, right, up, down):
    b0, b1, b2, b1d, b2r = fields
    return b0 * b, b1 * up(b) + b2 * left(b), b0 * a, b1d * down(a) + b2r * right(a)


def kernel(
    gxn, gyn, vec, bonds, onsite, out_mom, lbuf, rbuf,
    x, f, fd, c_own, c_left, c_right, halo_f, halo_x, keep, acc, part_mom,
    load_sem, send_sem, recv_sem, msend_sem, mrecv_sem,
):
    vectors, _, _, rows, cols = vec.shape
    tall = x.shape[3]
    tiles = cols // LANES
    last = rows - EDGE
    gx = lax.axis_index("gx")
    gy = lax.axis_index("gy")

    def peer(dx, dy):
        return (lax.rem(gx + dx + gxn, gxn), lax.rem(gy + dy + gyn, gyn))

    barrier = pltpu.get_barrier_semaphore()
    near = [(dx % gxn, dy % gyn) for dx in (-1, 0, 1) for dy in (-1, 0, 1)]
    near += [(0, dy) for dy in range(gyn)]
    near = sorted(set(near) - {(0, 0)})
    for dx, dy in near:
        pl.semaphore_signal(barrier, inc=1, device_id=peer(dx, dy), device_id_type=MESH)

    loads = [
        pltpu.make_async_copy(vec, x.at[:, :, :, 0:rows, :], load_sem.at[0]),
        pltpu.make_async_copy(bonds, f.at[0:3, 0:rows, :], load_sem.at[1]),
        pltpu.make_async_copy(onsite, f.at[3:5, 0:rows, :], load_sem.at[2]),
    ]
    for copy in loads:
        copy.start()
    sends = []

    def send(src, dst, dx, dy):
        n = len(sends)
        copy = pltpu.make_async_remote_copy(
            src_ref=src, dst_ref=dst, send_sem=send_sem.at[n], recv_sem=recv_sem.at[n],
            device_id=peer(dx, dy), device_id_type=MESH,
        )
        copy.start()
        sends.append(copy)

    for copy in loads:
        copy.wait()

    acc[...] = jnp.zeros_like(acc)
    pl.semaphore_wait(barrier, len(near))

    core = slice(0, rows)
    send(x.at[:, :, 0, 0:2, :], x.at[:, :, 0, rows : rows + 2, :], -1, 0)
    send(x.at[:, :, 1, rows - 2 : rows, :], x.at[:, :, 1, tall - 2 : tall, :], 1, 0)
    send(x.at[:, :, 1, 0:1, :], x.at[:, :, 1, rows : rows + 1, :], -1, 0)
    send(x.at[:, :, 0, rows - 1 : rows, :], x.at[:, :, 0, tall - 1 : tall, :], 1, 0)
    send(f.at[:, 0:2, :], f.at[:, rows : rows + 2, :], -1, 0)
    send(f.at[:, rows - 2 : rows, :], f.at[:, tall - 2 : tall, :], 1, 0)

    lane = lax.broadcasted_iota(jnp.int32, (rows, LANES), 1)
    spot = lax.rem(lane, HALF)

    def packed(items):
        total = jnp.zeros((rows, LANES), jnp.float32)
        for k, (first, final) in enumerate(items):
            both = jnp.where(lane < HALF, first, final)
            moved = pltpu.roll(both, GROUP * k + EDGE, 1)
            total = jnp.where(spot // GROUP == k, moved, total) if k else moved
        total = jnp.where(lane < HALF, total, pltpu.roll(total, HALF, 1))
        return total

    def edges(ref, *index):
        return ref[(*index, slice(0, rows), slice(0, LANES))], ref[
            (*index, slice(0, rows), slice(cols - LANES, cols))
        ]

    for sub in range(2):
        c_own[sub, 0:rows] = packed(
            [edges(x, v, p, sub) for v in range(vectors) for p in range(2)]
        )
    c_own[2, 0:rows] = packed([edges(f, k) for k in range(5)])

    send(c_own.at[:, core, :], c_right.at[:, core, :], 0, -1)
    send(c_own.at[:, core, :], c_left.at[:, core, :], 0, 1)
    top, bottom = c_own.at[:, 0:EDGE, :], c_own.at[:, last:rows, :]
    past, ahead = slice(rows, rows + EDGE), slice(tall - EDGE, tall)
    send(top, c_own.at[:, past, :], -1, 0)
    send(top, c_right.at[:, past, :], -1, -1)
    send(top, c_left.at[:, past, :], -1, 1)
    send(bottom, c_own.at[:, ahead, :], 1, 0)
    send(bottom, c_right.at[:, ahead, :], 1, -1)
    send(bottom, c_left.at[:, ahead, :], 1, 1)

    for copy in sends:
        copy.wait_recv()

    tlane = lax.broadcasted_iota(jnp.int32, (tall, LANES), 1)
    tspot = lax.rem(tlane, GROUP)
    from_left = (tlane < HALF) & (tspot < EDGE)
    from_right = (tlane >= HALF) & (tspot >= EDGE)

    def joined(k):
        return jnp.where(
            from_left, c_left[k], jnp.where(from_right, c_right[k], c_own[k])
        )

    def up(t):
        return pltpu.roll(t, 1, 0)

    def down(t):
        return pltpu.roll(t, t.shape[0] - 1, 0)

    field_tile = joined(2)
    tgroup = lax.rem(tlane, HALF)
    for k in range(5):
        t = pltpu.roll(field_tile, LANES - GROUP * k, 1) if k else field_tile
        t = jnp.where(tgroup < GROUP, t, 0.0)
        step = GROUP
        while step < HALF:
            t = t + pltpu.roll(t, step, 1)
            step *= 2
        halo_f[k] = t
    halo_f[5] = down(halo_f[1])
    halo_f[6] = pltpu.roll(halo_f[2], LANES - 1, 1)

    lane_last = tlane == LANES - 1
    lane_first = tlane == 0

    def tile(t):
        return slice(t * LANES, (t + 1) * LANES)

    for t in range(tiles):
        fd[0, :, tile(t)] = down(f[1, :, tile(t)])
    after = pltpu.roll(halo_f[2], LANES - 1 - (HALF + EDGE), 1)
    for t in reversed(range(tiles)):
        turned = pltpu.roll(f[2, :, tile(t)], LANES - 1, 1)
        fd[1, :, tile(t)] = jnp.where(lane_last, after, turned)
        after = turned

    sixth = 1.0 / SCALE

    def h_fields(width=tall):
        return tuple(halo_f[k] for k in (0, 1, 2, 5, 6))

    h_on = (halo_f[3], halo_f[4])

    def h_terms(a, b):
        return bond_terms(
            a, b, h_fields(), lambda t: pltpu.roll(t, 1, 1),
            lambda t: pltpu.roll(t, LANES - 1, 1), up, down,
        )

    def energy(a, b, terms, on, factor):
        a0, a12, b0, b12 = terms
        return (on[0] * a + (a0 + a12)) * factor, (on[1] * b + (b0 + b12)) * factor

    def speed(terms):
        a0, a12, b0, b12 = terms
        return a0 - 0.5 * a12, 0.5 * b12 - b0

    q0 = (joined(0), joined(1))
    t0 = h_terms(*q0)
    q1 = energy(*q0, t0, h_on, sixth)
    m0 = speed(t0)
    h1 = energy(*q1, h_terms(*q1), h_on, 2.0 * sixth)
    q2 = (h1[0] - q0[0], h1[1] - q0[1])
    m1 = energy(*m0, h_terms(*m0), h_on, sixth)
    for k, pair in enumerate((q0, q1, q2, m0, m1)):
        halo_x[k, 0], halo_x[k, 1] = pair

    short = slice(0, rows)

    def one_vector(v, carry):
        for part in range(2):
            turn_b = lax.rem(2 * LANES - (GROUP * (2 * v + part) + 1), LANES)
            turn_a = lax.rem(3 * LANES - 1 - (HALF + GROUP * (2 * v + part) + EDGE), LANES)

            def terms(pair, k, cut):
                a, b = pair
                rim_b = pltpu.roll(halo_x[k, 1], turn_b, 1)
                rim_a = pltpu.roll(halo_x[k, 0], turn_a, 1)
                keep_rows = (lambda t: t[0:rows]) if cut else (lambda t: t)
                first, final = keep_rows(lane_first), keep_rows(lane_last)
                size = short if cut else slice(0, tall)
                b_turn = [pltpu.roll(keep_rows(t), 1, 1) for t in b]
                a_turn = [pltpu.roll(keep_rows(t), LANES - 1, 1) for t in a]
                found = []
                for t in range(tiles):
                    prev = keep_rows(rim_b) if t == 0 else b_turn[t - 1]
                    nxt = keep_rows(rim_a) if t == tiles - 1 else a_turn[t + 1]
                    left = jnp.where(first, prev, b_turn[t])
                    right = jnp.where(final, nxt, a_turn[t])
                    a0 = f[0, size, tile(t)] * keep_rows(b[t])
                    a12 = f[1, size, tile(t)] * keep_rows(up(b[t])) + f[2, size, tile(t)] * left
                    b0 = f[0, size, tile(t)] * keep_rows(a[t])
                    b12 = fd[0, size, tile(t)] * keep_rows(down(a[t])) + fd[1, size, tile(t)] * right
                    found.append((a0, a12, b0, b12))
                return found

            def stepped(pair, found, factor, cut, minus=None):
                a_new, b_new = [], []
                size = short if cut else slice(0, tall)
                for t in range(tiles):
                    on = (f[3, size, tile(t)], f[4, size, tile(t)])
                    a, b = energy(pair[0][t][size], pair[1][t][size], found[t], on, factor)
                    if minus is not None:
                        a, b = a - minus[0][t][size], b - minus[1][t][size]
                    a_new.append(a)
                    b_new.append(b)
                return a_new, b_new

            def moved(found):
                both = [speed(item) for item in found]
                return [item[0] for item in both], [item[1] for item in both]

            def store(slot, pair):
                for sub in range(2):
                    for t in range(tiles):
                        keep[slot, part, sub, :, tile(t)] = pair[sub][t][0:rows]

            q0 = tuple([x[v, part, sub, :, tile(t)] for t in range(tiles)] for sub in range(2))
            t0 = terms(q0, 0, False)
            m0 = moved(t0)
            store(0, m0)
            q1 = stepped(q0, t0, sixth, False)
            t1 = terms(q1, 1, False)
            store(3, moved(t1))
            q2 = stepped(q1, t1, 2.0 * sixth, False, q0)
            n2 = moved(terms(q2, 2, True))
            store(4, n2)
            m1 = stepped(m0, terms(m0, 3, False), sixth, False)
            store(1, m1)
            m2 = stepped(m1, terms(m1, 4, True), 2.0 * sixth, True, m0)
            store(2, m2)
            for sub in range(2):
                for t in range(tiles):
                    for buf, pair in ((lbuf, m2), (rbuf, n2)):
                        value = pair[sub][t]
                        value = -value if part == 0 else value
                        buf[v, 1 - part, sub, :, tile(t)] = value.astype(jnp.bfloat16)

        for r in range(0, rows, 8):
            band = slice(r, r + 8)
            sums = [[[acc[p, n, m, band, :] for m in range(MOMENTS)] for n in range(MOMENTS)] for p in range(2)]
            for sub in range(2):
                for t in range(tiles):
                    at = [[keep[s, p, sub, band, tile(t)] for p in range(2)] for s in range(5)]
                    for n in range(MOMENTS):
                        for m in range(MOMENTS):
                            left = at[n]
                            right = at[0] if m == 0 else at[2 + m]
                            sums[0][n][m] = sums[0][n][m] + (left[0] * right[0] + left[1] * right[1])
                            sums[1][n][m] = sums[1][n][m] + (left[0] * right[1] - left[1] * right[0])
            for p in range(2):
                for n in range(MOMENTS):
                    for m in range(MOMENTS):
                        acc[p, n, m, band, :] = sums[p][n][m]
        return carry

    lax.fori_loop(0, vectors, one_vector, 0)

    count = 2 * MOMENTS * MOMENTS * rows
    part_mom[0] = lax.dot_general(
        jnp.ones((8, LANES), jnp.float32), acc[...].reshape(count, LANES),
        (((1,), (1,)), ((), ())), precision=lax.Precision.HIGHEST,
        preferred_element_type=jnp.float32,
    )
    swaps = []
    for d in range(1, gyn):
        copy = pltpu.make_async_remote_copy(
            src_ref=part_mom.at[0, 0:1], dst_ref=part_mom.at[d, 0:1],
            send_sem=msend_sem.at[d - 1], recv_sem=mrecv_sem.at[d - 1],
            device_id=peer(0, d), device_id_type=MESH,
        )
        copy.start()
        swaps.append(copy)
    for copy in swaps:
        copy.wait_recv()
    total = part_mom[0]
    for d in range(1, gyn):
        total = total + part_mom[d]
    out_mom[...] = total / float(vectors * cols * gyn)
    for copy in sends + swaps:
        copy.wait_send()


def writer(total, lbuf, rbuf, out_mom, out_left, out_right, out_sem):
    outs = [
        pltpu.make_async_copy(lbuf, out_left, out_sem.at[0]),
        pltpu.make_async_copy(rbuf, out_right, out_sem.at[1]),
    ]
    for copy in outs:
        copy.start()
    rows = out_mom.shape[3]
    for p in range(2):
        for n in range(MOMENTS):
            for m in range(MOMENTS):
                k = (p * MOMENTS + n) * MOMENTS + m
                out_mom[n, m, p : p + 1, :] = total[0:1, k * rows : (k + 1) * rows]
    for copy in outs:
        copy.wait()


def solution(mesh):
    gxn, gyn = mesh.shape["gx"], mesh.shape["gy"]

    def per_device(vectors, bonds, onsite):
        count, _, _, rows, cols = vectors.shape
        tall = rows + 8
        f32 = jnp.float32
        in_hbm = pl.BlockSpec(memory_space=pltpu.HBM)
        last = jax.ShapeDtypeStruct(vectors.shape, jnp.bfloat16)
        sends = 16
        in_vmem = pl.BlockSpec(memory_space=pltpu.VMEM)
        sums = (8, 2 * MOMENTS * MOMENTS * rows)
        made = pl.pallas_call(
            functools.partial(kernel, gxn, gyn),
            out_shape=(
                pltpu.VMEM(sums, f32),
                pltpu.VMEM(vectors.shape, jnp.bfloat16),
                pltpu.VMEM(vectors.shape, jnp.bfloat16),
            ),
            in_specs=[in_hbm] * 3,
            out_specs=(in_vmem,) * 3,
            scratch_shapes=[
                pltpu.VMEM((count, 2, 2, tall, cols), f32),
                pltpu.VMEM((5, tall, cols), f32),
                pltpu.VMEM((2, tall, cols), f32),
                pltpu.VMEM((3, tall, LANES), f32),
                pltpu.VMEM((3, tall, LANES), f32),
                pltpu.VMEM((3, tall, LANES), f32),
                pltpu.VMEM((7, tall, LANES), f32),
                pltpu.VMEM((5, 2, tall, LANES), f32),
                pltpu.VMEM((5, 2, 2, rows, cols), f32),
                pltpu.VMEM((2, MOMENTS, MOMENTS, rows, LANES), f32),
                pltpu.VMEM((gyn, *sums), f32),
                pltpu.SemaphoreType.DMA((3,)),
                pltpu.SemaphoreType.DMA((sends,)),
                pltpu.SemaphoreType.DMA((sends,)),
                pltpu.SemaphoreType.DMA((gyn - 1,)),
                pltpu.SemaphoreType.DMA((gyn - 1,)),
            ],
            compiler_params=pltpu.CompilerParams(
                collective_id=0, has_side_effects=True, vmem_limit_bytes=GRANT
            ),
        )(*(pltpu.with_memory_space_constraint(array, pltpu.HBM) for array in (vectors, bonds, onsite)))
        made = [pltpu.with_memory_space_constraint(array, pltpu.VMEM) for array in made]
        moments, left, right = pl.pallas_call(
            writer,
            out_shape=(
                jax.ShapeDtypeStruct((MOMENTS, MOMENTS, 2, rows), f32), last, last,
            ),
            in_specs=[in_vmem] * 3,
            out_specs=(in_vmem, in_hbm, in_hbm),
            scratch_shapes=[pltpu.SemaphoreType.DMA((2,))],
            compiler_params=pltpu.CompilerParams(vmem_limit_bytes=GRANT),
        )(*made)
        return jnp.transpose(moments, (2, 0, 1, 3)), left, right

    return jax.shard_map(
        per_device,
        mesh=mesh,
        in_specs=(P(None, None, None, "gx", "gy"), P(None, "gx", "gy"), P(None, "gx", "gy")),
        out_specs=(
            P(None, None, None, "gx"),
            P(None, None, None, "gx", "gy"),
            P(None, None, None, "gx", "gy"),
        ),
        check_vma=False,
    )
```

```python
import functools
import jax
import jax.numpy as jnp
from jax import lax
from jax.experimental import pallas as pl
from jax.experimental.pallas import tpu as pltpu
from jax.sharding import PartitionSpec as P

MOMENTS = 3
SCALE = 6.0
EDGE = 2
GROUP = 4
HALF = 64
LANES = 128
GRANT = 16 * 1024 * 1024
MESH = pl.DeviceIdType.MESH


def bond_terms(a, b, fields, left, right, up, down):
    b0, b1, b2, b1d, b2r = fields
    return b0 * b, b1 * up(b) + b2 * left(b), b0 * a, b1d * down(a) + b2r * right(a)


def kernel(
    gxn, gyn, vec, bonds, onsite, out_mom, lbuf, rbuf,
    x, f, fd, g, c_own, c_left, c_right, halo_f, halo_x, keep, acc, part_mom,
    load_sem, send_sem, recv_sem, msend_sem, mrecv_sem,
):
    vectors, _, _, rows, cols = vec.shape
    tall = x.shape[3]
    tiles = cols // LANES
    last = rows - EDGE
    gx = lax.axis_index("gx")
    gy = lax.axis_index("gy")

    def peer(dx, dy):
        return (lax.rem(gx + dx + gxn, gxn), lax.rem(gy + dy + gyn, gyn))

    barrier = pltpu.get_barrier_semaphore()
    near = [(dx % gxn, dy % gyn) for dx in (-1, 0, 1) for dy in (-1, 0, 1)]
    near += [(0, dy) for dy in range(gyn)]
    near = sorted(set(near) - {(0, 0)})
    for dx, dy in near:
        pl.semaphore_signal(barrier, inc=1, device_id=peer(dx, dy), device_id_type=MESH)

    loads = [
        pltpu.make_async_copy(vec, x.at[:, :, :, 0:rows, :], load_sem.at[0]),
        pltpu.make_async_copy(bonds, f.at[0:3, 0:rows, :], load_sem.at[1]),
        pltpu.make_async_copy(onsite, f.at[3:5, 0:rows, :], load_sem.at[2]),
    ]
    for copy in loads:
        copy.start()
    sends = []

    def send(src, dst, dx, dy):
        n = len(sends)
        copy = pltpu.make_async_remote_copy(
            src_ref=src, dst_ref=dst, send_sem=send_sem.at[n], recv_sem=recv_sem.at[n],
            device_id=peer(dx, dy), device_id_type=MESH,
        )
        copy.start()
        sends.append(copy)

    for copy in loads:
        copy.wait()

    acc[...] = jnp.zeros_like(acc)
    pl.semaphore_wait(barrier, len(near))

    core = slice(0, rows)
    send(x.at[:, :, 0, 0:2, :], x.at[:, :, 0, rows : rows + 2, :], -1, 0)
    send(x.at[:, :, 1, rows - 2 : rows, :], x.at[:, :, 1, tall - 2 : tall, :], 1, 0)
    send(x.at[:, :, 1, 0:1, :], x.at[:, :, 1, rows : rows + 1, :], -1, 0)
    send(x.at[:, :, 0, rows - 1 : rows, :], x.at[:, :, 0, tall - 1 : tall, :], 1, 0)
    send(f.at[:, 0:2, :], f.at[:, rows : rows + 2, :], -1, 0)
    send(f.at[:, rows - 2 : rows, :], f.at[:, tall - 2 : tall, :], 1, 0)

    lane = lax.broadcasted_iota(jnp.int32, (rows, LANES), 1)
    spot = lax.rem(lane, HALF)

    def packed(items):
        total = jnp.zeros((rows, LANES), jnp.float32)
        for k, (first, final) in enumerate(items):
            both = jnp.where(lane < HALF, first, final)
            moved = pltpu.roll(both, GROUP * k + EDGE, 1)
            total = jnp.where(spot // GROUP == k, moved, total) if k else moved
        total = jnp.where(lane < HALF, total, pltpu.roll(total, HALF, 1))
        return total

    def edges(ref, *index):
        return ref[(*index, slice(0, rows), slice(0, LANES))], ref[
            (*index, slice(0, rows), slice(cols - LANES, cols))
        ]

    for sub in range(2):
        c_own[sub, 0:rows] = packed(
            [edges(x, v, p, sub) for v in range(vectors) for p in range(2)]
        )
    c_own[2, 0:rows] = packed([edges(f, k) for k in range(5)])

    send(c_own.at[:, core, :], c_right.at[:, core, :], 0, -1)
    send(c_own.at[:, core, :], c_left.at[:, core, :], 0, 1)
    top, bottom = c_own.at[:, 0:EDGE, :], c_own.at[:, last:rows, :]
    past, ahead = slice(rows, rows + EDGE), slice(tall - EDGE, tall)
    send(top, c_own.at[:, past, :], -1, 0)
    send(top, c_right.at[:, past, :], -1, -1)
    send(top, c_left.at[:, past, :], -1, 1)
    send(bottom, c_own.at[:, ahead, :], 1, 0)
    send(bottom, c_right.at[:, ahead, :], 1, -1)
    send(bottom, c_left.at[:, ahead, :], 1, 1)

    for copy in sends:
        copy.wait_recv()

    tlane = lax.broadcasted_iota(jnp.int32, (tall, LANES), 1)
    tspot = lax.rem(tlane, GROUP)
    from_left = (tlane < HALF) & (tspot < EDGE)
    from_right = (tlane >= HALF) & (tspot >= EDGE)

    def joined(k):
        return jnp.where(
            from_left, c_left[k], jnp.where(from_right, c_right[k], c_own[k])
        )

    def up(t):
        return pltpu.roll(t, 1, 0)

    def down(t):
        return pltpu.roll(t, t.shape[0] - 1, 0)

    field_tile = joined(2)
    tgroup = lax.rem(tlane, HALF)
    for k in range(5):
        t = pltpu.roll(field_tile, LANES - GROUP * k, 1) if k else field_tile
        t = jnp.where(tgroup < GROUP, t, 0.0)
        step = GROUP
        while step < HALF:
            t = t + pltpu.roll(t, step, 1)
            step *= 2
        halo_f[k] = t
    halo_f[5] = down(halo_f[1])
    halo_f[6] = pltpu.roll(halo_f[2], LANES - 1, 1)

    lane_last = tlane == LANES - 1
    lane_first = tlane == 0

    def tile(t):
        return slice(t * LANES, (t + 1) * LANES)

    for t in range(tiles):
        fd[0, :, tile(t)] = down(f[1, :, tile(t)])
    after = pltpu.roll(halo_f[2], LANES - 1 - (HALF + EDGE), 1)
    for t in reversed(range(tiles)):
        turned = pltpu.roll(f[2, :, tile(t)], LANES - 1, 1)
        fd[1, :, tile(t)] = jnp.where(lane_last, after, turned)
        after = turned

    sixth = 1.0 / SCALE
    half_square = 0.5 * SCALE * SCALE
    for t in range(tiles):
        raw = [f[i, :, tile(t)] for i in range(3)] + [fd[i, :, tile(t)] for i in range(2)]
        raw += [f[i, :, tile(t)] for i in (3, 4)]
        for i, item in enumerate(raw):
            g[0, i, :, tile(t)] = item * sixth
            g[1, i, :, tile(t)] = item * (2.0 * sixth)
            if i < 5:
                g[2, i, :, tile(t)] = item * ((-0.5 if i in (1, 2, 3, 4) else 1.0) / half_square)

    def h_fields(width=tall):
        return tuple(halo_f[k] for k in (0, 1, 2, 5, 6))

    h_on = (halo_f[3], halo_f[4])

    def h_terms(a, b):
        return bond_terms(
            a, b, h_fields(), lambda t: pltpu.roll(t, 1, 1),
            lambda t: pltpu.roll(t, LANES - 1, 1), up, down,
        )

    def energy(a, b, terms, on, factor):
        a0, a12, b0, b12 = terms
        return (on[0] * a + (a0 + a12)) * factor, (on[1] * b + (b0 + b12)) * factor

    def speed(terms):
        a0, a12, b0, b12 = terms
        return a0 - 0.5 * a12, 0.5 * b12 - b0

    q0 = (joined(0), joined(1))
    t0 = h_terms(*q0)
    q1 = energy(*q0, t0, h_on, 1.0)
    m0 = speed(t0)
    h1 = energy(*q1, h_terms(*q1), h_on, 1.0)
    q2 = (h1[0] - half_square * q0[0], h1[1] - half_square * q0[1])
    m1 = energy(*m0, h_terms(*m0), h_on, sixth)
    for k, pair in enumerate((q0, q1, q2, m0, m1)):
        halo_x[k, 0], halo_x[k, 1] = pair

    short = slice(0, rows)

    def one_vector(v, carry):
        for part in range(2):
            turn_b = lax.rem(2 * LANES - (GROUP * (2 * v + part) + 1), LANES)
            turn_a = lax.rem(3 * LANES - 1 - (HALF + GROUP * (2 * v + part) + EDGE), LANES)

            def terms(pair, k, cut, w=None):
                a, b = pair
                rim_b = pltpu.roll(halo_x[k, 1], turn_b, 1)
                rim_a = pltpu.roll(halo_x[k, 0], turn_a, 1)
                keep_rows = (lambda t: t[0:rows]) if cut else (lambda t: t)
                first, final = keep_rows(lane_first), keep_rows(lane_last)
                size = short if cut else slice(0, tall)
                b_turn = [pltpu.roll(keep_rows(t), 1, 1) for t in b]
                a_turn = [pltpu.roll(keep_rows(t), LANES - 1, 1) for t in a]
                found = []
                for t in range(tiles):
                    prev = keep_rows(rim_b) if t == 0 else b_turn[t - 1]
                    nxt = keep_rows(rim_a) if t == tiles - 1 else a_turn[t + 1]
                    left = jnp.where(first, prev, b_turn[t])
                    right = jnp.where(final, nxt, a_turn[t])
                    if w is None:
                        f0, f1, f2 = (f[i, size, tile(t)] for i in range(3))
                        d1, d2 = fd[0, size, tile(t)], fd[1, size, tile(t)]
                    else:
                        f0, f1, f2, d1, d2 = (g[w, i, size, tile(t)] for i in range(5))
                    a0 = f0 * keep_rows(b[t])
                    a12 = f1 * keep_rows(up(b[t])) + f2 * left
                    b0 = f0 * keep_rows(a[t])
                    b12 = d1 * keep_rows(down(a[t])) + d2 * right
                    found.append((a0, a12, b0, b12))
                return found

            def stepped(pair, found, cut, w=None, minus=None, times=None):
                a_new, b_new = [], []
                size = short if cut else slice(0, tall)
                for t in range(tiles):
                    if w is None:
                        on = (f[3, size, tile(t)], f[4, size, tile(t)])
                    else:
                        on = (g[w, 5, size, tile(t)], g[w, 6, size, tile(t)])
                    a0, a12, b0, b12 = found[t]
                    a = on[0] * pair[0][t][size] + (a0 + a12)
                    b = on[1] * pair[1][t][size] + (b0 + b12)
                    if minus is not None:
                        less = [minus[i][t][size] for i in range(2)]
                        if times is not None:
                            less = [item * times for item in less]
                        a, b = a - less[0], b - less[1]
                    a_new.append(a)
                    b_new.append(b)
                return a_new, b_new

            def moved(found):
                both = [speed(item) for item in found]
                return [item[0] for item in both], [item[1] for item in both]

            def store(slot, pair):
                for sub in range(2):
                    for t in range(tiles):
                        keep[slot, part, sub, :, tile(t)] = pair[sub][t][0:rows]

            q0 = tuple([x[v, part, sub, :, tile(t)] for t in range(tiles)] for sub in range(2))
            t0 = terms(q0, 0, False)
            m0 = moved(t0)
            store(0, m0)
            q1 = stepped(q0, t0, False)
            t1 = terms(q1, 1, False)
            store(3, moved(t1))
            q2 = stepped(q1, t1, False, None, q0, half_square)
            n2 = [[], []]
            for a0, a12, b0, b12 in terms(q2, 2, True, 2):
                n2[0].append(a0 + a12)
                n2[1].append(-(b0 + b12))
            store(4, n2)
            m1 = stepped(m0, terms(m0, 3, False, 0), False, 0)
            store(1, m1)
            m2 = stepped(m1, terms(m1, 4, True, 1), True, 1, m0)
            store(2, m2)
            for sub in range(2):
                for t in range(tiles):
                    for buf, pair in ((lbuf, m2), (rbuf, n2)):
                        value = pair[sub][t]
                        value = -value if part == 0 else value
                        buf[v, 1 - part, sub, :, tile(t)] = value.astype(jnp.bfloat16)

        for r in range(0, rows, 8):
            band = slice(r, r + 8)
            sums = [[[acc[p, n, m, band, :] for m in range(MOMENTS)] for n in range(MOMENTS)] for p in range(2)]
            for sub in range(2):
                for t in range(tiles):
                    at = [[keep[s, p, sub, band, tile(t)] for p in range(2)] for s in range(5)]
                    for n in range(MOMENTS):
                        for m in range(MOMENTS):
                            left = at[n]
                            right = at[0] if m == 0 else at[2 + m]
                            sums[0][n][m] = sums[0][n][m] + (left[0] * right[0] + left[1] * right[1])
                            sums[1][n][m] = sums[1][n][m] + (left[0] * right[1] - left[1] * right[0])
            for p in range(2):
                for n in range(MOMENTS):
                    for m in range(MOMENTS):
                        acc[p, n, m, band, :] = sums[p][n][m]
        return carry

    lax.fori_loop(0, vectors, one_vector, 0)

    for p in range(2):
        for n in range(MOMENTS):
            acc[p, n, 1] = acc[p, n, 1] * sixth
    count = 2 * MOMENTS * MOMENTS * rows
    part_mom[0] = lax.dot_general(
        jnp.ones((8, LANES), jnp.float32), acc[...].reshape(count, LANES),
        (((1,), (1,)), ((), ())), precision=lax.Precision.HIGHEST,
        preferred_element_type=jnp.float32,
    )
    swaps = []
    for d in range(1, gyn):
        copy = pltpu.make_async_remote_copy(
            src_ref=part_mom.at[0, 0:1], dst_ref=part_mom.at[d, 0:1],
            send_sem=msend_sem.at[d - 1], recv_sem=mrecv_sem.at[d - 1],
            device_id=peer(0, d), device_id_type=MESH,
        )
        copy.start()
        swaps.append(copy)
    for copy in swaps:
        copy.wait_recv()
    total = part_mom[0]
    for d in range(1, gyn):
        total = total + part_mom[d]
    out_mom[...] = total / float(vectors * cols * gyn)
    for copy in sends + swaps:
        copy.wait_send()


def writer(total, lbuf, rbuf, out_mom, out_left, out_right, out_sem):
    outs = [
        pltpu.make_async_copy(lbuf, out_left, out_sem.at[0]),
        pltpu.make_async_copy(rbuf, out_right, out_sem.at[1]),
    ]
    for copy in outs:
        copy.start()
    rows = out_mom.shape[3]
    for p in range(2):
        for n in range(MOMENTS):
            for m in range(MOMENTS):
                k = (p * MOMENTS + n) * MOMENTS + m
                out_mom[n, m, p : p + 1, :] = total[0:1, k * rows : (k + 1) * rows]
    for copy in outs:
        copy.wait()


def solution(mesh):
    gxn, gyn = mesh.shape["gx"], mesh.shape["gy"]

    def per_device(vectors, bonds, onsite):
        count, _, _, rows, cols = vectors.shape
        tall = rows + 8
        f32 = jnp.float32
        in_hbm = pl.BlockSpec(memory_space=pltpu.HBM)
        last = jax.ShapeDtypeStruct(vectors.shape, jnp.bfloat16)
        sends = 16
        in_vmem = pl.BlockSpec(memory_space=pltpu.VMEM)
        sums = (8, 2 * MOMENTS * MOMENTS * rows)
        made = pl.pallas_call(
            functools.partial(kernel, gxn, gyn),
            out_shape=(
                pltpu.VMEM(sums, f32),
                pltpu.VMEM(vectors.shape, jnp.bfloat16),
                pltpu.VMEM(vectors.shape, jnp.bfloat16),
            ),
            in_specs=[in_hbm] * 3,
            out_specs=(in_vmem,) * 3,
            scratch_shapes=[
                pltpu.VMEM((count, 2, 2, tall, cols), f32),
                pltpu.VMEM((5, tall, cols), f32),
                pltpu.VMEM((2, tall, cols), f32),
                pltpu.VMEM((3, 7, tall, cols), f32),
                pltpu.VMEM((3, tall, LANES), f32),
                pltpu.VMEM((3, tall, LANES), f32),
                pltpu.VMEM((3, tall, LANES), f32),
                pltpu.VMEM((7, tall, LANES), f32),
                pltpu.VMEM((5, 2, tall, LANES), f32),
                pltpu.VMEM((5, 2, 2, rows, cols), f32),
                pltpu.VMEM((2, MOMENTS, MOMENTS, rows, LANES), f32),
                pltpu.VMEM((gyn, *sums), f32),
                pltpu.SemaphoreType.DMA((3,)),
                pltpu.SemaphoreType.DMA((sends,)),
                pltpu.SemaphoreType.DMA((sends,)),
                pltpu.SemaphoreType.DMA((gyn - 1,)),
                pltpu.SemaphoreType.DMA((gyn - 1,)),
            ],
            compiler_params=pltpu.CompilerParams(
                collective_id=0, has_side_effects=True, vmem_limit_bytes=GRANT
            ),
        )(*(pltpu.with_memory_space_constraint(array, pltpu.HBM) for array in (vectors, bonds, onsite)))
        made = [pltpu.with_memory_space_constraint(array, pltpu.VMEM) for array in made]
        moments, left, right = pl.pallas_call(
            writer,
            out_shape=(
                jax.ShapeDtypeStruct((MOMENTS, MOMENTS, 2, rows), f32), last, last,
            ),
            in_specs=[in_vmem] * 3,
            out_specs=(in_vmem, in_hbm, in_hbm),
            scratch_shapes=[pltpu.SemaphoreType.DMA((2,))],
            compiler_params=pltpu.CompilerParams(vmem_limit_bytes=GRANT),
        )(*made)
        return jnp.transpose(moments, (2, 0, 1, 3)), left, right

    return jax.shard_map(
        per_device,
        mesh=mesh,
        in_specs=(P(None, None, None, "gx", "gy"), P(None, "gx", "gy"), P(None, "gx", "gy")),
        out_specs=(
            P(None, None, None, "gx"),
            P(None, None, None, "gx", "gy"),
            P(None, None, None, "gx", "gy"),
        ),
        check_vma=False,
    )
```

```python
import functools
import jax
import jax.numpy as jnp
from jax import lax
from jax.experimental import pallas as pl
from jax.experimental.pallas import tpu as pltpu
from jax.sharding import PartitionSpec as P

MOMENTS = 3
SCALE = 6.0
EDGE = 2
GROUP = 4
HALF = 64
LANES = 128
GRANT = 16 * 1024 * 1024
MESH = pl.DeviceIdType.MESH


def bond_terms(a, b, fields, left, right, up, down):
    b0, b1, b2, b1d, b2r = fields
    return b0 * b, b1 * up(b) + b2 * left(b), b0 * a, b1d * down(a) + b2r * right(a)


def kernel(
    gxn, gyn, vec, bonds, onsite, out_mom, lbuf, rbuf,
    x, f, fd, g, c_own, c_left, c_right, halo_f, halo_x, keep, acc, part_mom,
    load_sem, send_sem, recv_sem, msend_sem, mrecv_sem,
):
    vectors, _, _, rows, cols = vec.shape
    tall = x.shape[3]
    tiles = cols // LANES
    last = rows - EDGE
    gx = lax.axis_index("gx")
    gy = lax.axis_index("gy")

    def peer(dx, dy):
        return (lax.rem(gx + dx + gxn, gxn), lax.rem(gy + dy + gyn, gyn))

    barrier = pltpu.get_barrier_semaphore()
    near = [(dx % gxn, dy % gyn) for dx in (-1, 0, 1) for dy in (-1, 0, 1)]
    near += [(0, dy) for dy in range(gyn)]
    near = sorted(set(near) - {(0, 0)})
    for dx, dy in near:
        pl.semaphore_signal(barrier, inc=1, device_id=peer(dx, dy), device_id_type=MESH)

    loads = [
        pltpu.make_async_copy(vec, x.at[:, :, :, 0:rows, :], load_sem.at[0]),
        pltpu.make_async_copy(bonds, f.at[0:3, 0:rows, :], load_sem.at[1]),
        pltpu.make_async_copy(onsite, f.at[3:5, 0:rows, :], load_sem.at[2]),
    ]
    for copy in loads:
        copy.start()
    sends = []

    def send(src, dst, dx, dy):
        n = len(sends)
        copy = pltpu.make_async_remote_copy(
            src_ref=src, dst_ref=dst, send_sem=send_sem.at[n], recv_sem=recv_sem.at[n],
            device_id=peer(dx, dy), device_id_type=MESH,
        )
        copy.start()
        sends.append(copy)

    for copy in loads:
        copy.wait()

    acc[...] = jnp.zeros_like(acc)
    pl.semaphore_wait(barrier, len(near))

    core = slice(0, rows)
    send(x.at[:, :, 0, 0:2, :], x.at[:, :, 0, rows : rows + 2, :], -1, 0)
    send(x.at[:, :, 1, rows - 2 : rows, :], x.at[:, :, 1, tall - 2 : tall, :], 1, 0)
    send(x.at[:, :, 1, 0:1, :], x.at[:, :, 1, rows : rows + 1, :], -1, 0)
    send(x.at[:, :, 0, rows - 1 : rows, :], x.at[:, :, 0, tall - 1 : tall, :], 1, 0)
    send(f.at[:, 0:2, :], f.at[:, rows : rows + 2, :], -1, 0)
    send(f.at[:, rows - 2 : rows, :], f.at[:, tall - 2 : tall, :], 1, 0)

    lane = lax.broadcasted_iota(jnp.int32, (rows, LANES), 1)
    spot = lax.rem(lane, HALF)

    def packed(items):
        total = jnp.zeros((rows, LANES), jnp.float32)
        for k, (first, final) in enumerate(items):
            both = jnp.where(lane < HALF, first, final)
            moved = pltpu.roll(both, GROUP * k + EDGE, 1)
            total = jnp.where(spot // GROUP == k, moved, total) if k else moved
        total = jnp.where(lane < HALF, total, pltpu.roll(total, HALF, 1))
        return total

    def edges(ref, *index):
        return ref[(*index, slice(0, rows), slice(0, LANES))], ref[
            (*index, slice(0, rows), slice(cols - LANES, cols))
        ]

    for sub in range(2):
        c_own[sub, 0:rows] = packed(
            [edges(x, v, p, sub) for v in range(vectors) for p in range(2)]
        )
    c_own[2, 0:rows] = packed([edges(f, k) for k in range(5)])

    send(c_own.at[:, core, :], c_right.at[:, core, :], 0, -1)
    send(c_own.at[:, core, :], c_left.at[:, core, :], 0, 1)
    top, bottom = c_own.at[:, 0:EDGE, :], c_own.at[:, last:rows, :]
    past, ahead = slice(rows, rows + EDGE), slice(tall - EDGE, tall)
    send(top, c_own.at[:, past, :], -1, 0)
    send(top, c_right.at[:, past, :], -1, -1)
    send(top, c_left.at[:, past, :], -1, 1)
    send(bottom, c_own.at[:, ahead, :], 1, 0)
    send(bottom, c_right.at[:, ahead, :], 1, -1)
    send(bottom, c_left.at[:, ahead, :], 1, 1)

    def scaled(i, t, item):
        g[0, i, :, tile(t)] = item * (1.0 / SCALE)
        g[1, i, :, tile(t)] = item * (2.0 / SCALE)
        if i < 5:
            g[2, i, :, tile(t)] = item * ((-1.0 if i else 2.0) / (SCALE * SCALE))

    def tile(t):
        return slice(t * LANES, (t + 1) * LANES)

    for copy in sends[4:6]:
        copy.wait_recv()
    for t in range(tiles):
        fd[0, :, tile(t)] = pltpu.roll(f[1, :, tile(t)], tall - 1, 0)
        for i, item in ((0, f[0, :, tile(t)]), (1, f[1, :, tile(t)]), (2, f[2, :, tile(t)]),
                        (3, fd[0, :, tile(t)]), (5, f[3, :, tile(t)]), (6, f[4, :, tile(t)])):
            scaled(i, t, item)
    for copy in sends[:4] + sends[6:]:
        copy.wait_recv()

    tlane = lax.broadcasted_iota(jnp.int32, (tall, LANES), 1)
    tspot = lax.rem(tlane, GROUP)
    from_left = (tlane < HALF) & (tspot < EDGE)
    from_right = (tlane >= HALF) & (tspot >= EDGE)

    def joined(k):
        return jnp.where(
            from_left, c_left[k], jnp.where(from_right, c_right[k], c_own[k])
        )

    def up(t):
        return pltpu.roll(t, 1, 0)

    def down(t):
        return pltpu.roll(t, t.shape[0] - 1, 0)

    field_tile = joined(2)
    tgroup = lax.rem(tlane, HALF)
    for k in range(5):
        t = pltpu.roll(field_tile, LANES - GROUP * k, 1) if k else field_tile
        t = jnp.where(tgroup < GROUP, t, 0.0)
        step = GROUP
        while step < HALF:
            t = t + pltpu.roll(t, step, 1)
            step *= 2
        halo_f[k] = t
    halo_f[5] = down(halo_f[1])
    halo_f[6] = pltpu.roll(halo_f[2], LANES - 1, 1)

    lane_last = tlane == LANES - 1
    lane_first = tlane == 0

    def tile(t):
        return slice(t * LANES, (t + 1) * LANES)

    after = pltpu.roll(halo_f[2], LANES - 1 - (HALF + EDGE), 1)
    for t in reversed(range(tiles)):
        turned = pltpu.roll(f[2, :, tile(t)], LANES - 1, 1)
        fd[1, :, tile(t)] = jnp.where(lane_last, after, turned)
        after = turned

    sixth = 1.0 / SCALE
    half_square = 0.5 * SCALE * SCALE
    for t in range(tiles):
        scaled(4, t, fd[1, :, tile(t)])

    def h_fields(width=tall):
        return tuple(halo_f[k] for k in (0, 1, 2, 5, 6))

    h_on = (halo_f[3], halo_f[4])

    def h_terms(a, b):
        return bond_terms(
            a, b, h_fields(), lambda t: pltpu.roll(t, 1, 1),
            lambda t: pltpu.roll(t, LANES - 1, 1), up, down,
        )

    def energy(a, b, terms, on, factor):
        a0, a12, b0, b12 = terms
        return (on[0] * a + (a0 + a12)) * factor, (on[1] * b + (b0 + b12)) * factor

    def speed(terms):
        a0, a12, b0, b12 = terms
        return a0 - 0.5 * a12, 0.5 * b12 - b0

    q0 = (joined(0), joined(1))
    t0 = h_terms(*q0)
    q1 = energy(*q0, t0, h_on, 1.0)
    m0 = speed(t0)
    h1 = energy(*q1, h_terms(*q1), h_on, 1.0)
    q2 = (h1[0] - half_square * q0[0], h1[1] - half_square * q0[1])
    m1 = energy(*m0, h_terms(*m0), h_on, sixth)
    for k, pair in enumerate((q0, q1, q2, m0, m1)):
        halo_x[k, 0], halo_x[k, 1] = pair

    short = slice(0, rows)

    def one_vector(v, carry):
        for part in range(2):
            turn_b = lax.rem(2 * LANES - (GROUP * (2 * v + part) + 1), LANES)
            turn_a = lax.rem(3 * LANES - 1 - (HALF + GROUP * (2 * v + part) + EDGE), LANES)

            def terms(pair, k, cut, w=None):
                a, b = pair
                rim_b = pltpu.roll(halo_x[k, 1], turn_b, 1)
                rim_a = pltpu.roll(halo_x[k, 0], turn_a, 1)
                keep_rows = (lambda t: t[0:rows]) if cut else (lambda t: t)
                first, final = keep_rows(lane_first), keep_rows(lane_last)
                size = short if cut else slice(0, tall)
                b_turn = [pltpu.roll(keep_rows(t), 1, 1) for t in b]
                a_turn = [pltpu.roll(keep_rows(t), LANES - 1, 1) for t in a]
                found = []
                for t in range(tiles):
                    prev = keep_rows(rim_b) if t == 0 else b_turn[t - 1]
                    nxt = keep_rows(rim_a) if t == tiles - 1 else a_turn[t + 1]
                    left = jnp.where(first, prev, b_turn[t])
                    right = jnp.where(final, nxt, a_turn[t])
                    if w is None:
                        f0, f1, f2 = (f[i, size, tile(t)] for i in range(3))
                        d1, d2 = fd[0, size, tile(t)], fd[1, size, tile(t)]
                    else:
                        f0, f1, f2, d1, d2 = (g[w, i, size, tile(t)] for i in range(5))
                    a0 = f0 * keep_rows(b[t])
                    a12 = f1 * keep_rows(up(b[t])) + f2 * left
                    b0 = f0 * keep_rows(a[t])
                    b12 = d1 * keep_rows(down(a[t])) + d2 * right
                    found.append((a0, a12, b0, b12))
                return found

            def stepped(pair, found, cut, w=None, minus=None, times=None):
                a_new, b_new = [], []
                size = short if cut else slice(0, tall)
                for t in range(tiles):
                    if w is None:
                        on = (f[3, size, tile(t)], f[4, size, tile(t)])
                    else:
                        on = (g[w, 5, size, tile(t)], g[w, 6, size, tile(t)])
                    a0, a12, b0, b12 = found[t]
                    a = on[0] * pair[0][t][size] + (a0 + a12)
                    b = on[1] * pair[1][t][size] + (b0 + b12)
                    if minus is not None:
                        less = [minus[i][t][size] for i in range(2)]
                        if times is not None:
                            less = [item * times for item in less]
                        a, b = a - less[0], b - less[1]
                    a_new.append(a)
                    b_new.append(b)
                return a_new, b_new

            def moved(found):
                both = [speed(item) for item in found]
                return [item[0] for item in both], [item[1] for item in both]

            def store(slot, pair):
                for sub in range(2):
                    for t in range(tiles):
                        keep[slot, part, sub, :, tile(t)] = pair[sub][t][0:rows]

            q0 = tuple([x[v, part, sub, :, tile(t)] for t in range(tiles)] for sub in range(2))
            t0 = terms(q0, 0, False)
            m0 = moved(t0)
            store(0, m0)
            q1 = stepped(q0, t0, False)
            t1 = terms(q1, 1, False)
            store(3, moved(t1))
            q2 = stepped(q1, t1, False, None, q0, half_square)
            n2 = [[], []]
            for a0, a12, b0, b12 in terms(q2, 2, True, 2):
                n2[0].append(a0 + a12)
                n2[1].append(-(b0 + b12))
            store(4, n2)
            m1 = stepped(m0, terms(m0, 3, False, 0), False, 0)
            store(1, m1)
            m2 = stepped(m1, terms(m1, 4, True, 1), True, 1, m0)
            store(2, m2)
            for sub in range(2):
                for t in range(tiles):
                    for buf, pair in ((lbuf, m2), (rbuf, n2)):
                        value = pair[sub][t]
                        value = -value if part == 0 else value
                        buf[v, 1 - part, sub, :, tile(t)] = value.astype(jnp.bfloat16)

        for r in range(0, rows, 8):
            band = slice(r, r + 8)
            sums = [[[acc[p, n, m, band, :] for m in range(MOMENTS)] for n in range(MOMENTS)] for p in range(2)]
            for sub in range(2):
                for t in range(tiles):
                    at = [[keep[s, p, sub, band, tile(t)] for p in range(2)] for s in range(5)]
                    for n in range(MOMENTS):
                        for m in range(MOMENTS):
                            left = at[n]
                            right = at[0] if m == 0 else at[2 + m]
                            sums[0][n][m] = sums[0][n][m] + (left[0] * right[0] + left[1] * right[1])
                            sums[1][n][m] = sums[1][n][m] + (left[0] * right[1] - left[1] * right[0])
            for p in range(2):
                for n in range(MOMENTS):
                    for m in range(MOMENTS):
                        acc[p, n, m, band, :] = sums[p][n][m]
        return carry

    lax.fori_loop(0, vectors, one_vector, 0)

    for p in range(2):
        for n in range(MOMENTS):
            acc[p, n, 1] = acc[p, n, 1] * sixth
    count = 2 * MOMENTS * MOMENTS * rows
    part_mom[0] = lax.dot_general(
        jnp.ones((8, LANES), jnp.float32), acc[...].reshape(count, LANES),
        (((1,), (1,)), ((), ())), precision=lax.Precision.HIGHEST,
        preferred_element_type=jnp.float32,
    )
    swaps = []
    for d in range(1, gyn):
        copy = pltpu.make_async_remote_copy(
            src_ref=part_mom.at[0, 0:1], dst_ref=part_mom.at[d, 0:1],
            send_sem=msend_sem.at[d - 1], recv_sem=mrecv_sem.at[d - 1],
            device_id=peer(0, d), device_id_type=MESH,
        )
        copy.start()
        swaps.append(copy)
    for copy in swaps:
        copy.wait_recv()
    total = part_mom[0]
    for d in range(1, gyn):
        total = total + part_mom[d]
    out_mom[...] = total / float(vectors * cols * gyn)
    for copy in sends + swaps:
        copy.wait_send()


def writer(total, lbuf, rbuf, out_mom, out_left, out_right, out_sem):
    outs = [
        pltpu.make_async_copy(lbuf, out_left, out_sem.at[0]),
        pltpu.make_async_copy(rbuf, out_right, out_sem.at[1]),
    ]
    for copy in outs:
        copy.start()
    rows = out_mom.shape[3]
    for p in range(2):
        for n in range(MOMENTS):
            for m in range(MOMENTS):
                k = (p * MOMENTS + n) * MOMENTS + m
                out_mom[n, m, p : p + 1, :] = total[0:1, k * rows : (k + 1) * rows]
    for copy in outs:
        copy.wait()


def solution(mesh):
    gxn, gyn = mesh.shape["gx"], mesh.shape["gy"]

    def per_device(vectors, bonds, onsite):
        count, _, _, rows, cols = vectors.shape
        tall = rows + 8
        f32 = jnp.float32
        in_hbm = pl.BlockSpec(memory_space=pltpu.HBM)
        last = jax.ShapeDtypeStruct(vectors.shape, jnp.bfloat16)
        sends = 16
        in_vmem = pl.BlockSpec(memory_space=pltpu.VMEM)
        sums = (8, 2 * MOMENTS * MOMENTS * rows)
        made = pl.pallas_call(
            functools.partial(kernel, gxn, gyn),
            out_shape=(
                pltpu.VMEM(sums, f32),
                pltpu.VMEM(vectors.shape, jnp.bfloat16),
                pltpu.VMEM(vectors.shape, jnp.bfloat16),
            ),
            in_specs=[in_hbm] * 3,
            out_specs=(in_vmem,) * 3,
            scratch_shapes=[
                pltpu.VMEM((count, 2, 2, tall, cols), f32),
                pltpu.VMEM((5, tall, cols), f32),
                pltpu.VMEM((2, tall, cols), f32),
                pltpu.VMEM((3, 7, tall, cols), f32),
                pltpu.VMEM((3, tall, LANES), f32),
                pltpu.VMEM((3, tall, LANES), f32),
                pltpu.VMEM((3, tall, LANES), f32),
                pltpu.VMEM((7, tall, LANES), f32),
                pltpu.VMEM((5, 2, tall, LANES), f32),
                pltpu.VMEM((5, 2, 2, rows, cols), f32),
                pltpu.VMEM((2, MOMENTS, MOMENTS, rows, LANES), f32),
                pltpu.VMEM((gyn, *sums), f32),
                pltpu.SemaphoreType.DMA((3,)),
                pltpu.SemaphoreType.DMA((sends,)),
                pltpu.SemaphoreType.DMA((sends,)),
                pltpu.SemaphoreType.DMA((gyn - 1,)),
                pltpu.SemaphoreType.DMA((gyn - 1,)),
            ],
            compiler_params=pltpu.CompilerParams(
                collective_id=0, has_side_effects=True, vmem_limit_bytes=GRANT
            ),
        )(*(pltpu.with_memory_space_constraint(array, pltpu.HBM) for array in (vectors, bonds, onsite)))
        made = [pltpu.with_memory_space_constraint(array, pltpu.VMEM) for array in made]
        moments, left, right = pl.pallas_call(
            writer,
            out_shape=(
                jax.ShapeDtypeStruct((MOMENTS, MOMENTS, 2, rows), f32), last, last,
            ),
            in_specs=[in_vmem] * 3,
            out_specs=(in_vmem, in_hbm, in_hbm),
            scratch_shapes=[pltpu.SemaphoreType.DMA((2,))],
            compiler_params=pltpu.CompilerParams(vmem_limit_bytes=GRANT),
        )(*made)
        return jnp.transpose(moments, (2, 0, 1, 3)), left, right

    return jax.shard_map(
        per_device,
        mesh=mesh,
        in_specs=(P(None, None, None, "gx", "gy"), P(None, "gx", "gy"), P(None, "gx", "gy")),
        out_specs=(
            P(None, None, None, "gx"),
            P(None, None, None, "gx", "gy"),
            P(None, None, None, "gx", "gy"),
        ),
        check_vma=False,
    )
```
